256 devices in a mesh: gx: 32 (over x, z), gy: 8 (over y, core).
Axes of the slice: x: 4, y: 4, z: 8, core: 2. Of those that a mesh axis runs over, the one named last changes fastest.
Arguments:
- parcel_props: float32 [16, 1048576], P(None, ('gx', 'gy')), may hold values from -6 to 6
- size_class: int32 [1048576], P(('gx', 'gy')), may hold values from 0 to 7
- dest_owner: int32 [1048576, 1], P(('gx', 'gy')), may hold values from 0 to 255; in each aligned block of 4096 rows (0 to 4095, 4096 to 8191, ...) at most 64 rows name the same one
- dest_local: int32 [1048576], P(('gx', 'gy')), may hold values from 0 to 4095
- class_table: float32 [8, 16], replicated, may hold values from 0.5 to 2
- gas_density: float32 [1024, 1024], P('gx', 'gy'), may hold values from 0.5 to 2
- gas_rest: float32 [4, 1024, 1024], P(None, 'gx', 'gy'), may hold values from -6 to 6
Outputs:
- new_density: float32 [1024, 1024], P('gx', 'gy')
- new_rest: float32 [4, 1024, 1024], P(None, 'gx', 'gy')
The draws below stay inside these ranges and needn't reach their ends.
Inputs may be any that keep to these rules, and one draw needn't show every extreme that they name: `dest_owner`: among the parcels of one device, no owner device is named by more than 64 of them, a bound that some block reaches.
All inputs are finite; a program needn't handle non-finite values.
Results may differ from the reference program's by a relative error of at most 0.00015.
Values sent between devices are 32-bit elements; how exact they have to be, the bound alone decides.
A program may use at most 64 MiB of HBM per device.

```python
import math
import jax
import jax.numpy as jnp
import numpy as np
from jax import lax

PROPS = 16
CLASSES = 8
PARC_DEV = 4096
LX = 32
LY = 128
CAP = 64
PARCELS = 1048576
NX = 1024
NY = 1024
N_GY = 8
DEVICES = 256


def place_ends(drawn, rng, least, high):
    longest = drawn.shape.index(max(drawn.shape))
    spots = []
    for shift in (0, 1):
        where = [jax.random.randint(jax.random.fold_in(rng, axis), (), 0, length) for axis, length in enumerate(drawn.shape)]
        where[longest] = (where[longest] + shift) % drawn.shape[longest]
        spots.append(tuple(where))
    return drawn.at[spots[0]].set(least).at[spots[1]].set(high)


def steps_of(own_key, shape, shards, least, largest):
    def one(axis_at, shards_of):
        heights = jax.random.uniform(jax.random.fold_in(jax.random.fold_in(own_key, 6), axis_at), (shards_of,), jnp.float32, least / len(shards), largest / len(shards))
        return jnp.repeat(jnp.exp(heights), shape[axis_at] // shards_of).reshape((-1,) + (1,) * (len(shape) - axis_at - 1))

    level = one(*shards[0])
    for cut in shards[1:]:
        level = level * one(*cut)
    return level


def routed_block(key, own, number, rows, count, top, limit, lean):
    sequence = jax.random.permutation(key, count)
    packed, common = load_shares(count, rows * top, limit, lean, True), load_shares(count, rows * top, limit, lean, False)
    places = jnp.arange(count)

    def named(tallies, rotation):
        used = int((tallies > 0).sum())
        fixed = max(1, used // 4)
        shifted = fixed + (places - fixed + rotation * (used - fixed)) % max(1, count - fixed)
        return jnp.zeros((count,), jnp.int32).at[sequence[jnp.where(places < fixed, places, shifted)]].set(jnp.asarray(tallies, jnp.int32))

    tallies = jnp.where(number % 4 == 0, named(packed, number // 4), named(common, number - number // 4 - 1))
    mixed = jax.random.permutation(jax.random.fold_in(own, 3), count)
    source_of, sink = mixed[0:count // 2 * 2:2], mixed[1:count // 2 * 2:2]
    margin = jnp.minimum(tallies[source_of] - 1, limit - tallies[sink]) // 2
    margin = jnp.where((source_of == sequence[0]) | (sink == sequence[0]) | (tallies[sink] == 0), 0, jnp.maximum(margin, 0))
    shifted = jax.random.randint(jax.random.fold_in(own, 4), (count // 2,), 0, 1 << 20) % (margin + 1)
    tallies = tallies.at[source_of].add(-shifted).at[sink].add(shifted)
    members = jnp.searchsorted(jnp.cumsum(tallies), jnp.arange(rows * top), side="right").astype(jnp.int32)
    table = members.reshape(top, rows).T
    table = table[jax.random.permutation(jax.random.fold_in(own, 1), rows)]
    rotation = jax.random.randint(jax.random.fold_in(own, 2), (rows, 1), 0, top)
    return jnp.take_along_axis(table, (jnp.arange(top)[None, :] + rotation) % top, axis=1)


def load_shares(count, total, most, lean, full):
    weights = [(1 << 20) // math.isqrt(standing ** lean) + 1 for standing in range(1, count + 1)]
    largest = most if full else min(most, max(-(-total // count), total * weights[0] // sum(weights)))
    least = 1 if total - largest >= count - 1 else 0
    holding, surplus = [largest] + [least] * (count - 1), total - largest - least * (count - 1)
    while surplus > 0:
        free = [i for i in range(1, count) if holding[i] < largest] or [i for i in range(1, count) if holding[i] < most]
        whole, left = sum([weights[i] for i in free]), surplus
        for i in free:
            more = min(most - holding[i], max(1, left * weights[i] // whole), surplus)
            holding[i] = holding[i] + more
            surplus = surplus - more
    return np.array(holding)


def bell_draw(key, extent, width, most, cuts=(), kind=jnp.bfloat16):
    array = width * jax.random.normal(key, extent, jnp.float32)
    if cuts:
        array = array * steps_of(key, extent, cuts, -0.22, 0.18)
    return jnp.clip(array, -most, most).astype(kind)


def setup_inputs(seed: int = 0) -> dict:
    seeds = jax.random.split(jax.random.key(seed), 8)
    parcel_props = bell_draw(seeds[0], (PROPS, PARCELS), 1.0, 6.0, ((1, 256),), jnp.float32)
    size_class = place_ends(jax.random.randint(seeds[1], (PARCELS,), 0, CLASSES), jax.random.fold_in(seeds[1], 1), 0, CLASSES - 1).astype(jnp.int32)
    dest_owner_keys = jax.random.split(jax.random.fold_in(seeds[2], 1), PARCELS // PARC_DEV)
    dest_owner_turns = jax.random.permutation(jax.random.fold_in(seeds[2], 3), PARCELS // PARC_DEV)
    dest_owner = jax.vmap(lambda own, number: routed_block(jax.random.fold_in(seeds[2], 2), own, number, PARC_DEV, DEVICES, 1, CAP, 2))(dest_owner_keys, dest_owner_turns).reshape((PARCELS, 1))
    dest_local = place_ends(jax.random.randint(seeds[3], (PARCELS,), 0, LX * LY), jax.random.fold_in(seeds[3], 1), 0, (LX * LY) - 1).astype(jnp.int32)
    class_table = jnp.clip(jnp.exp(jax.random.uniform(seeds[4], (CLASSES, PROPS), jnp.float32, math.log(0.5), math.log(2.0))), 0.5, 2.0)
    gas_density = jnp.clip(jnp.exp(math.log(2.0) - 1.3862944 * jax.random.uniform(seeds[5], (NX, NY), jnp.float32) ** steps_of(seeds[5], (NX, NY), ((0, 32), (1, 8)), -0.2, 0.2)), 0.5, 2.0)
    gas_rest = bell_draw(seeds[6], (4, NX, NY), 1.0, 6.0, ((1, 32), (2, 8)), jnp.float32)
    return dict(parcel_props=parcel_props, size_class=size_class, dest_owner=dest_owner, dest_local=dest_local, class_table=class_table, gas_density=gas_density, gas_rest=gas_rest)


def sources_of(props, classes, gas, table):
    picks = (classes[None, :] == jnp.arange(CLASSES, dtype=jnp.int32)[:, None]).astype(jnp.float32)
    coef = jnp.dot(table.T, picks, precision=lax.Precision.HIGHEST, preferred_element_type=jnp.float32)
    mass = jnp.exp(0.5 * props[0])
    density = gas[0]
    velocity = gas[1:4] / density
    theta = gas[4] / density
    slip = props[1:4] - velocity
    rate = coef[0] * jax.nn.softplus(props[4] - theta)
    evapor = mass * (1.0 - jnp.exp(-rate))
    dragged = 1.0 - jnp.exp(-coef[1] * jnp.sqrt(1.0 + lax.optimization_barrier(jnp.sum(slip * slip, axis=0))))
    moment = evapor * coef[2:5] * props[1:4] + mass * dragged * slip
    energy = evapor * (props[4] + lax.optimization_barrier(jnp.sum(coef[5:] * props[5:], axis=0)))
    return jnp.concatenate([evapor[None], moment, energy[None]], axis=0)

def smooth_field(deposit):
    padded = jnp.pad(deposit, ((0, 0), (1, 1), (1, 1)))
    beside = padded[:, 2:, 1:-1] + padded[:, :-2, 1:-1] + padded[:, 1:-1, 2:] + padded[:, 1:-1, :-2]
    return 0.4 * deposit + 0.15 * beside

def reference(parcel_props, size_class, dest_owner, dest_local, class_table, gas_density, gas_rest):
    owner = dest_owner[:, 0]
    cell_x = owner // N_GY * LX + dest_local // LY
    cell_y = owner % N_GY * LY + dest_local % LY
    flat = (cell_x * NY + cell_y).astype(jnp.int32)
    gas = jnp.concatenate([gas_density[None], gas_rest], axis=0).reshape(5, NX * NY)
    local_gas = gas[:, flat]
    source = sources_of(parcel_props, size_class, local_gas, class_table)
    deposit = jnp.zeros((5, NX * NY), jnp.float32).at[:, flat].add(source).reshape(5, NX, NY)
    smooth = smooth_field(deposit)
    return (gas_density + smooth[0], gas_rest + smooth[1:])
```

```python
import functools

import jax
import jax.numpy as jnp
from jax import lax
from jax.experimental import pallas as pl
from jax.experimental.pallas import tpu as pltpu
from jax.sharding import PartitionSpec as P

MESH = pl.DeviceIdType.MESH
F32 = jnp.float32
BF16 = jnp.bfloat16

X, Z, Y, CORES = 4, 8, 4, 2
DEVICES = X * Z * Y * CORES
PARCELS = 4096
CAP = 64
LX, LY = 32, 128
WORDS = 8
STEP = 256
GROUPS = 8
GROUP = DEVICES // GROUPS


def offsets():
    far = [
        (dx, dz, dy, dc)
        for dy in range(Y)
        for dc in range(CORES)
        for dx in range(X)
        for dz in (4, 1, 7, 2, 6, 3, 5, 0)
        if dx or dz or dy or dc
    ]
    return [(0, 0, 0, 0)] + far


def here():
    gx = lax.axis_index("gx")
    gy = lax.axis_index("gy")
    return gx // Z, gx % Z, gy // CORES, gy % CORES


def peer(at, dx, dz, dy, dc):
    x, z, y, core = at
    return (((x + dx) % X) * Z + (z + dz) % Z, ((y + dy) % Y) * CORES + (core + dc) % CORES)


def signal(sem, to):
    pl.semaphore_signal(sem, inc=1, device_id=to, device_id_type=MESH)


def in_row(at):
    return [peer(at, 0, 0, dy, dc) for dy in range(Y) for dc in range(CORES) if dy or dc]


def in_column(at):
    return [peer(at, dx, dz, 0, 0) for dx in range(X) for dz in range(Z) if dx or dz]


def two_parts(v):
    high = v.astype(BF16).astype(F32)
    return high, v - high


def iota(shape, dim):
    return lax.broadcasted_iota(jnp.int32, shape, dim)


def wide_row(ref, step):
    return jnp.concatenate([ref[2 * step : 2 * step + 1], ref[2 * step + 1 : 2 * step + 2]], axis=1)


def spread(row, height):
    part = jnp.broadcast_to(row, (16, row.shape[1])).astype(BF16)
    return jnp.concatenate([part] * (height // 16), axis=0)


def dot_last(a, b):
    return lax.dot_general(a, b, (((1,), (1,)), ((), ())), preferred_element_type=F32)


def pack(props, classes, owners, locals_, table, blocks, packed):
    across = iota((STEP, STEP), 1)
    down = iota((STEP, STEP), 0)
    earlier = (down < across).astype(F32).astype(BF16)
    ones = jnp.ones((STEP, 128), BF16)
    carry = jnp.zeros((DEVICES, 128), F32)
    columns = jnp.transpose(jnp.concatenate([table[...], jnp.zeros((8, 112), F32)], axis=1))[:16]
    columns = [jnp.broadcast_to(columns[:, k : k + 1], (16, STEP)) for k in range(8)]
    for step in range(PARCELS // STEP):
        owner = wide_row(owners, step)
        mine = down == owner
        member = jnp.where(mine, 1.0, 0.0).astype(BF16)
        before = jnp.dot(member, earlier, preferred_element_type=F32)
        before = before + jnp.concatenate([carry, carry], axis=1)
        rank = jnp.sum(jnp.where(mine, before, 0.0), axis=0, keepdims=True)
        carry = carry + jnp.dot(member, ones, preferred_element_type=F32)

        q = props[:, step * STEP : (step + 1) * STEP]
        kind = wide_row(classes, step)
        coef = columns[0]
        for k in range(1, 8):
            coef = jnp.where(kind == k, columns[k], coef)
        made = jnp.where(iota((16, STEP), 0) >= 5, coef * q, 0.0)
        energy = q[4:5] + jnp.sum(made, axis=0, keepdims=True)
        local = wide_row(locals_, step).astype(F32)
        words = [q[0:1], q[1:2], q[2:3], q[3:4], q[4:5], energy, kind.astype(F32) + 1.0, local]

        hot = jnp.where(iota((CAP, STEP), 0).astype(F32) == rank, 1.0, 0.0).astype(BF16)
        parts = [two_parts(w) for w in words]
        held = [hot * spread(p[0], CAP) for p in parts] + [hot * spread(p[1], CAP) for p in parts]
        placed = dot_last(jnp.concatenate(held, axis=0), member)
        placed = placed[: WORDS * CAP] + placed[WORDS * CAP :]
        if step:
            packed[...] += placed
        else:
            packed[...] = placed
    for j in range(WORDS // 2):
        blocks[:, j, :] = jnp.transpose(packed[128 * j : 128 * j + 128, :])


def look_up(gas_rows, hi, lo):
    found = [jnp.zeros(hi.shape, F32) for _ in range(5)]
    for h in range(LX):
        at = hi == h
        for k in range(5):
            row = jnp.broadcast_to(gas_rows(k, h), hi.shape)
            found[k] = jnp.where(at, jnp.take_along_axis(row, lo, axis=1, mode="promise_in_bounds"), found[k])
    return found


def sources(words, gas, table):
    q0, q1, q2, q3, q4, energy, kind, _ = words
    coef = []
    for j in range(5):
        c = jnp.full(q0.shape, table[0, j], F32)
        for k in range(1, 8):
            c = jnp.where(kind == k + 1.0, table[k, j], c)
        coef.append(c)
    mass = jnp.where(kind > 0.5, jnp.exp(0.5 * q0), 0.0)
    inverse = 1.0 / gas[0]
    slip = [q - m * inverse for q, m in zip((q1, q2, q3), gas[1:4])]
    warm = q4 - gas[4] * inverse
    rate = coef[0] * (jnp.maximum(warm, 0.0) + jnp.log1p(jnp.exp(-jnp.abs(warm))))
    evapor = mass * (1.0 - jnp.exp(-rate))
    speed = 1.0 + slip[0] * slip[0] + slip[1] * slip[1] + slip[2] * slip[2]
    dragged = mass * (1.0 - jnp.exp(-coef[1] * jnp.sqrt(speed)))
    moment = [evapor * c * q + dragged * w for c, q, w in zip(coef[2:5], (q1, q2, q3), slip)]
    return [evapor, *moment, evapor * energy]


def receive_group(group, recv, gas_rows, table, dense, deposit):
    lane = iota((8, 128), 1)
    for half in range(GROUP // 16):
        first = group * GROUP + 16 * half
        words = []
        for j in range(WORDS // 2):
            a = recv[first : first + 8, j, :]
            b = recv[first + 8 : first + 16, j, :]
            words.append(jnp.where(lane < 64, a, pltpu.roll(b, 64, 1)))
            words.append(jnp.where(lane < 64, pltpu.roll(a, 64, 1), b))
        cell = words[7].astype(jnp.int32)
        hi, lo = cell >> 7, cell & 127
        src = sources(words, look_up(gas_rows, hi, lo), table)
        rows = slice(8 * half, 8 * half + 8)
        for k in range(5):
            dense[2 * k, rows], dense[2 * k + 1, rows] = two_parts(src[k])
        dense[10, rows] = hi.astype(F32)
        dense[11, rows] = lo.astype(F32)
    total = jnp.zeros((320, LY), F32)
    for step in range(GROUP * CAP // STEP):
        at_hi = jnp.where(iota((LX, STEP), 0).astype(F32) == wide_row(dense.at[10], step), 1.0, 0.0).astype(BF16)
        at_lo = jnp.where(iota((LY, STEP), 0).astype(F32) == wide_row(dense.at[11], step), 1.0, 0.0).astype(BF16)
        held = [at_hi * spread(wide_row(dense.at[2 * k + p], step), LX) for p in (0, 1) for k in range(5)]
        total = total + dot_last(jnp.concatenate(held, axis=0), at_lo)
    total = total[:160] + total[160:]
    if group:
        deposit[...] += total
    else:
        deposit[...] = total


def kernel(
    props, classes, owners, locals_, table, table_s, density, rest,
    new_density, new_rest,
    blocks, packed, recv, dense, deposit, edges, halo,
    second, send_sem, recv_sem, edge_sem, halo_sem,
):
    at = here()
    gx, gy = lax.axis_index("gx"), lax.axis_index("gy")
    barrier = pltpu.get_barrier_semaphore()
    row, column = in_row(at), in_column(at)
    for to in row + column:
        signal(barrier, to)

    pack(props, classes, owners, locals_, table, blocks, packed)

    pl.semaphore_wait(barrier, len(row) + len(column))
    for to in row:
        signal(second, to)
    pl.semaphore_wait(second, len(row))

    order = offsets()
    for slot, off in enumerate(order):
        if slot:
            to = peer(at, *off)
            pltpu.make_async_remote_copy(
                src_ref=blocks.at[to[0] * 8 + to[1]],
                dst_ref=recv.at[slot],
                send_sem=send_sem,
                recv_sem=recv_sem.at[slot // GROUP],
                device_id=to,
                device_id_type=MESH,
            ).start()
    recv[0] = blocks[gx * 8 + gy]

    def gas_rows(k, h):
        return density[h : h + 1] if k == 0 else rest[k - 1, h : h + 1]

    def arrived(copies, sem):
        pltpu.make_async_copy(blocks.at[:copies], recv.at[:copies], sem).wait()

    for group in range(GROUPS):
        arrived(GROUP if group else GROUP - 1, recv_sem.at[group])
        receive_group(group, recv, gas_rows, table_s, dense, deposit)
    arrived(DEVICES - 1, send_sem)

    lane = iota((8, 128), 1)
    low_column = jnp.zeros((8, 128), F32)
    high_column = jnp.zeros((8, 128), F32)
    for i in range(20):
        tile = deposit[8 * i : 8 * i + 8]
        low_column = jnp.where(lane == i, pltpu.roll(tile, i, 1) if i else tile, low_column)
        high_column = jnp.where(lane == i, pltpu.roll(tile, i + 1, 1), high_column)
    pad = jnp.zeros((3, 128), F32)
    edges[0] = jnp.concatenate([deposit[32 * k : 32 * k + 1] for k in range(5)] + [pad], axis=0)
    edges[1] = jnp.concatenate([deposit[32 * k + 31 : 32 * k + 32] for k in range(5)] + [pad], axis=0)
    edges[2] = low_column
    edges[3] = high_column
    beside = [
        ((gx + 31) % 32, gy),
        ((gx + 1) % 32, gy),
        (gx, (gy + 7) % 8),
        (gx, (gy + 1) % 8),
    ]
    copies = [
        pltpu.make_async_remote_copy(
            src_ref=edges.at[i],
            dst_ref=halo.at[i],
            send_sem=edge_sem.at[i],
            recv_sem=halo_sem.at[i],
            device_id=to,
            device_id_type=MESH,
        )
        for i, to in enumerate(beside)
    ]
    for copy in copies:
        copy.start()
    for copy in copies:
        copy.wait()

    def kept(value, there):
        return jnp.where(there, value, 0.0)

    above = kept(halo[0], gx < 31)
    below = kept(halo[1], gx > 0)
    right = kept(halo[2], gy < 7)
    left = kept(halo[3], gy > 0)
    for k in range(5):
        field = deposit[32 * k : 32 * k + 32]
        up = jnp.concatenate([field[1:], above[k : k + 1]], axis=0)
        down = jnp.concatenate([below[k : k + 1], field[:-1]], axis=0)
        rights, lefts = [], []
        for i in range(4 * k, 4 * k + 4):
            tile = deposit[8 * i : 8 * i + 8]
            rights.append(jnp.where(lane == 127, pltpu.roll(right, 127 - i, 1), pltpu.roll(tile, 127, 1)))
            lefts.append(jnp.where(lane == 0, pltpu.roll(left, 128 - i, 1) if i else left, pltpu.roll(tile, 1, 1)))
        around = up + down + jnp.concatenate(rights, axis=0) + jnp.concatenate(lefts, axis=0)
        smooth = 0.4 * field + 0.15 * around
        if k == 0:
            new_density[...] = density[...] + smooth
        else:
            new_rest[k - 1] = rest[k - 1] + smooth


def per_device(parcel_props, size_class, dest_owner, dest_local, class_table, gas_density, gas_rest):
    vmem = pl.BlockSpec(memory_space=pltpu.VMEM)
    smem = pl.BlockSpec(memory_space=pltpu.SMEM)
    return pl.pallas_call(
        kernel,
        out_shape=(
            jax.ShapeDtypeStruct((LX, LY), F32),
            jax.ShapeDtypeStruct((4, LX, LY), F32),
        ),
        in_specs=[vmem, vmem, vmem, vmem, vmem, smem, vmem, vmem],
        out_specs=(vmem, vmem),
        scratch_shapes=[
            pltpu.VMEM((DEVICES, WORDS // 2, 128), F32),
            pltpu.VMEM((WORDS * CAP, DEVICES), F32),
            pltpu.VMEM((DEVICES, WORDS // 2, 128), F32),
            pltpu.VMEM((12, GROUP // 2, 128), F32),
            pltpu.VMEM((160, LY), F32),
            pltpu.VMEM((4, 8, 128), F32),
            pltpu.VMEM((4, 8, 128), F32),
            pltpu.SemaphoreType.REGULAR,
            pltpu.SemaphoreType.DMA,
            pltpu.SemaphoreType.DMA((GROUPS,)),
            pltpu.SemaphoreType.DMA((4,)),
            pltpu.SemaphoreType.DMA((4,)),
        ],
        compiler_params=pltpu.CompilerParams(collective_id=0, has_side_effects=True),
    )(
        parcel_props,
        size_class.reshape(32, 128),
        dest_owner.reshape(32, 128),
        dest_local.reshape(32, 128),
        class_table,
        class_table,
        gas_density,
        gas_rest,
    )


def solution(mesh):
    return jax.shard_map(
        per_device,
        mesh=mesh,
        in_specs=(
            P(None, ("gx", "gy")),
            P(("gx", "gy")),
            P(("gx", "gy"), None),
            P(("gx", "gy")),
            P(),
            P("gx", "gy"),
            P(None, "gx", "gy"),
        ),
        out_specs=(P("gx", "gy"), P(None, "gx", "gy")),
        check_vma=False,
    )
```

```python
import jax
import jax.numpy as jnp
from jax import lax
from jax.experimental import pallas as pl
from jax.experimental.pallas import tpu as pltpu
from jax.sharding import PartitionSpec as P

MESH = pl.DeviceIdType.MESH
F32 = jnp.float32
BF16 = jnp.bfloat16

X, Z, Y, CORES = 4, 8, 4, 2
DEVICES = X * Z * Y * CORES
PARCELS = 4096
CAP = 64
LX, LY = 32, 128
WORDS = 8
STEP = 256
GROUPS = 8
GROUP = DEVICES // GROUPS


PLANES = (0, 1, 7, 2, 6, 3, 5, 4)


def offsets():
    flat = [(dx, dy, dc) for dx in range(X) for dy in range(Y) for dc in range(CORES)]
    return [(dx, dz, dy, dc) for dz in PLANES for dx, dy, dc in flat]


def here():
    gx = lax.axis_index("gx")
    gy = lax.axis_index("gy")
    return gx // Z, gx % Z, gy // CORES, gy % CORES


def peer(at, dx, dz, dy, dc):
    x, z, y, core = at
    return (((x + dx) % X) * Z + (z + dz) % Z, ((y + dy) % Y) * CORES + (core + dc) % CORES)


def signal(sem, to):
    pl.semaphore_signal(sem, inc=1, device_id=to, device_id_type=MESH)


def in_plane(at):
    flat = [(dx, dy, dc) for dx in range(X) for dy in range(Y) for dc in range(CORES)]
    return [peer(at, dx, 0, dy, dc) for dx, dy, dc in flat if dx or dy or dc]


def two_parts(v):
    high = v.astype(BF16).astype(F32)
    return high, v - high


def iota(shape, dim):
    return lax.broadcasted_iota(jnp.int32, shape, dim)


def wide_row(ref, step):
    return jnp.concatenate([ref[2 * step : 2 * step + 1], ref[2 * step + 1 : 2 * step + 2]], axis=1)


def spread(row, height):
    part = jnp.broadcast_to(row, (16, row.shape[1])).astype(BF16)
    return jnp.concatenate([part] * (height // 16), axis=0)


def dot_last(a, b):
    return lax.dot_general(a, b, (((1,), (1,)), ((), ())), preferred_element_type=F32)


def pack(props, classes, owners, locals_, table, blocks, packed, midway):
    across = iota((STEP, STEP), 1)
    down = iota((STEP, STEP), 0)
    earlier = (down < across).astype(F32).astype(BF16)
    ones = jnp.ones((STEP, 128), BF16)
    carry = jnp.zeros((DEVICES, 128), F32)
    columns = jnp.transpose(jnp.concatenate([table[...], jnp.zeros((8, 112), F32)], axis=1))[:16]
    columns = [jnp.broadcast_to(columns[:, k : k + 1], (16, STEP)) for k in range(8)]
    for step in range(PARCELS // STEP):
        if step == 10:
            midway()
        owner = wide_row(owners, step)
        mine = down == owner
        member = jnp.where(mine, 1.0, 0.0).astype(BF16)
        before = jnp.dot(member, earlier, preferred_element_type=F32)
        before = before + jnp.concatenate([carry, carry], axis=1)
        rank = jnp.sum(jnp.where(mine, before, 0.0), axis=0, keepdims=True)
        carry = carry + jnp.dot(member, ones, preferred_element_type=F32)

        q = props[:, step * STEP : (step + 1) * STEP]
        kind = wide_row(classes, step)
        coef = columns[0]
        for k in range(1, 8):
            coef = jnp.where(kind == k, columns[k], coef)
        made = jnp.where(iota((16, STEP), 0) >= 5, coef * q, 0.0)
        energy = q[4:5] + jnp.sum(made, axis=0, keepdims=True)
        local = wide_row(locals_, step).astype(F32)
        words = [q[0:1], q[1:2], q[2:3], q[3:4], q[4:5], energy, kind.astype(F32) + 1.0, local]

        hot = jnp.where(iota((CAP, STEP), 0).astype(F32) == rank, 1.0, 0.0).astype(BF16)
        parts = [two_parts(w) for w in words]
        held = [hot * spread(p[0], CAP) for p in parts] + [hot * spread(p[1], CAP) for p in parts]
        placed = dot_last(jnp.concatenate(held, axis=0), member)
        placed = placed[: WORDS * CAP] + placed[WORDS * CAP :]
        if step:
            packed[...] += placed
        else:
            packed[...] = placed
    for j in range(WORDS // 2):
        blocks[:, j, :] = jnp.transpose(packed[128 * j : 128 * j + 128, :])


def look_up(gas_rows, hi, lo):
    found = [jnp.zeros(hi.shape, F32) for _ in range(5)]
    for h in range(LX):
        at = hi == h
        for k in range(5):
            row = jnp.broadcast_to(gas_rows(k, h), hi.shape)
            found[k] = jnp.where(at, jnp.take_along_axis(row, lo, axis=1, mode="promise_in_bounds"), found[k])
    return found


def sources(words, gas, table):
    q0, q1, q2, q3, q4, energy, kind, _ = words
    coef = []
    for j in range(5):
        c = jnp.full(q0.shape, table[0, j], F32)
        for k in range(1, 8):
            c = jnp.where(kind == k + 1.0, table[k, j], c)
        coef.append(c)
    mass = jnp.where(kind > 0.5, jnp.exp(0.5 * q0), 0.0)
    inverse = 1.0 / gas[0]
    slip = [q - m * inverse for q, m in zip((q1, q2, q3), gas[1:4])]
    warm = q4 - gas[4] * inverse
    rate = coef[0] * (jnp.maximum(warm, 0.0) + jnp.log1p(jnp.exp(-jnp.abs(warm))))
    evapor = mass * (1.0 - jnp.exp(-rate))
    speed = 1.0 + slip[0] * slip[0] + slip[1] * slip[1] + slip[2] * slip[2]
    dragged = mass * (1.0 - jnp.exp(-coef[1] * jnp.sqrt(speed)))
    moment = [evapor * c * q + dragged * w for c, q, w in zip(coef[2:5], (q1, q2, q3), slip)]
    return [evapor, *moment, evapor * energy]


def find_sources(group, recv, gas_rows, table, dense):
    lane = iota((8, 128), 1)
    for half in range(GROUP // 16):
        first = group * GROUP + 16 * half
        words = []
        for j in range(WORDS // 2):
            a = recv[first : first + 8, j, :]
            b = recv[first + 8 : first + 16, j, :]
            words.append(jnp.where(lane < 64, a, pltpu.roll(b, 64, 1)))
            words.append(jnp.where(lane < 64, pltpu.roll(a, 64, 1), b))
        cell = words[7].astype(jnp.int32)
        hi, lo = cell >> 7, cell & 127
        src = sources(words, look_up(gas_rows, hi, lo), table)
        rows = slice(8 * half, 8 * half + 8)
        for k in range(5):
            dense[2 * k, rows], dense[2 * k + 1, rows] = two_parts(src[k])
        dense[10, rows] = hi.astype(F32)
        dense[11, rows] = lo.astype(F32)


def add_sources(group, dense, deposit):
    total = jnp.zeros((320, LY), F32)
    for step in range(GROUP * CAP // STEP):
        at_hi = jnp.where(iota((LX, STEP), 0).astype(F32) == wide_row(dense.at[10], step), 1.0, 0.0).astype(BF16)
        at_lo = jnp.where(iota((LY, STEP), 0).astype(F32) == wide_row(dense.at[11], step), 1.0, 0.0).astype(BF16)
        held = [at_hi * spread(wide_row(dense.at[2 * k + p], step), LX) for p in (0, 1) for k in range(5)]
        total = total + dot_last(jnp.concatenate(held, axis=0), at_lo)
    total = total[:160] + total[160:]
    if group:
        deposit[...] += total
    else:
        deposit[...] = total


def kernel(
    props_h, classes_h, owners_h, locals_h, table, table_s, density_h, rest_h,
    new,
    props, classes, owners, locals_, density, rest, blocks, packed, recv, dense, deposit, edges, halo,
    load_sem, ready, send_sem, recv_sem, edge_sem, halo_sem,
):
    loads = [
        pltpu.make_async_copy(src, dst, load_sem.at[i])
        for i, (src, dst) in enumerate(
            [(owners_h, owners), (props_h, props), (classes_h, classes), (locals_h, locals_), (density_h, density), (rest_h, rest)]
        )
    ]
    for load in loads:
        load.start()
    at = here()
    gx, gy = lax.axis_index("gx"), lax.axis_index("gy")
    barrier = pltpu.get_barrier_semaphore()
    plane = in_plane(at)
    column = [peer(at, 0, dz, 0, 0) for dz in range(1, Z)]
    for to in column + plane:
        signal(barrier, to)

    for load in loads:
        load.wait()

    def midway():
        pl.semaphore_wait(barrier, len(plane) + len(column))
        for dz in range(1, Z):
            signal(ready.at[dz], column[dz - 1])

    pack(props, classes, owners, locals_, table, blocks, packed, midway)

    for slot, off in enumerate(offsets()):
        to = peer(at, *off)
        if slot % GROUP == 0 and off[1]:
            pl.semaphore_wait(ready.at[Z - off[1]], 1)
        if off == (0, 0, 0, 0):
            recv[slot] = blocks[gx * 8 + gy]
        else:
            pltpu.make_async_remote_copy(
                src_ref=blocks.at[to[0] * 8 + to[1]],
                dst_ref=recv.at[slot],
                send_sem=send_sem,
                recv_sem=recv_sem.at[slot // GROUP],
                device_id=to,
                device_id_type=MESH,
            ).start()

    def gas_rows(k, h):
        return density[h : h + 1] if k == 0 else rest[k - 1, h : h + 1]

    def arrived(copies, sem):
        pltpu.make_async_copy(blocks.at[:copies], recv.at[:copies], sem).wait()

    for group in range(GROUPS):
        arrived(GROUP if PLANES[group] else GROUP - 1, recv_sem.at[group])
        if group:
            add_sources(group - 1, dense.at[(group - 1) % 2], deposit)
        find_sources(group, recv, gas_rows, table_s, dense.at[group % 2])
    add_sources(GROUPS - 1, dense.at[(GROUPS - 1) % 2], deposit)
    arrived(DEVICES - 1, send_sem)

    lane = iota((8, 128), 1)
    low_column = jnp.zeros((8, 128), F32)
    high_column = jnp.zeros((8, 128), F32)
    for i in range(20):
        tile = deposit[8 * i : 8 * i + 8]
        low_column = jnp.where(lane == i, pltpu.roll(tile, i, 1) if i else tile, low_column)
        high_column = jnp.where(lane == i, pltpu.roll(tile, i + 1, 1), high_column)
    pad = jnp.zeros((3, 128), F32)
    edges[0] = jnp.concatenate([deposit[32 * k : 32 * k + 1] for k in range(5)] + [pad], axis=0)
    edges[1] = jnp.concatenate([deposit[32 * k + 31 : 32 * k + 32] for k in range(5)] + [pad], axis=0)
    edges[2] = low_column
    edges[3] = high_column
    beside = [
        ((gx + 31) % 32, gy),
        ((gx + 1) % 32, gy),
        (gx, (gy + 7) % 8),
        (gx, (gy + 1) % 8),
    ]
    copies = [
        pltpu.make_async_remote_copy(
            src_ref=edges.at[i],
            dst_ref=halo.at[i],
            send_sem=edge_sem.at[i],
            recv_sem=halo_sem.at[i],
            device_id=to,
            device_id_type=MESH,
        )
        for i, to in enumerate(beside)
    ]
    for copy in copies:
        copy.start()
    for copy in copies:
        copy.wait()

    def kept(value, there):
        return jnp.where(there, value, 0.0)

    above = kept(halo[0], gx < 31)
    below = kept(halo[1], gx > 0)
    right = kept(halo[2], gy < 7)
    left = kept(halo[3], gy > 0)
    for k in range(5):
        field = deposit[32 * k : 32 * k + 32]
        up = jnp.concatenate([field[1:], above[k : k + 1]], axis=0)
        down = jnp.concatenate([below[k : k + 1], field[:-1]], axis=0)
        rights, lefts = [], []
        for i in range(4 * k, 4 * k + 4):
            tile = deposit[8 * i : 8 * i + 8]
            rights.append(jnp.where(lane == 127, pltpu.roll(right, 127 - i, 1), pltpu.roll(tile, 127, 1)))
            lefts.append(jnp.where(lane == 0, pltpu.roll(left, 128 - i, 1) if i else left, pltpu.roll(tile, 1, 1)))
        around = up + down + jnp.concatenate(rights, axis=0) + jnp.concatenate(lefts, axis=0)
        smooth = 0.4 * field + 0.15 * around
        gas = density[...] if k == 0 else rest[k - 1]
        new[k] = gas + smooth


def put_out(new, new_density, new_rest, sem):
    copies = [
        pltpu.make_async_copy(new.at[0], new_density, sem.at[0]),
        pltpu.make_async_copy(new.at[1:], new_rest, sem.at[1]),
    ]
    for copy in copies:
        copy.start()
    for copy in copies:
        copy.wait()


def per_device(parcel_props, size_class, dest_owner, dest_local, class_table, gas_density, gas_rest):
    vmem = pl.BlockSpec(memory_space=pltpu.VMEM)
    hbm = pl.BlockSpec(memory_space=pltpu.HBM)
    smem = pl.BlockSpec(memory_space=pltpu.SMEM)
    new = pl.pallas_call(
        kernel,
        out_shape=jax.ShapeDtypeStruct((5, LX, LY), F32),
        in_specs=[hbm, hbm, hbm, hbm, vmem, smem, hbm, hbm],
        out_specs=vmem,
        scratch_shapes=[
            pltpu.VMEM((16, PARCELS), F32),
            pltpu.VMEM((32, 128), jnp.int32),
            pltpu.VMEM((32, 128), jnp.int32),
            pltpu.VMEM((32, 128), jnp.int32),
            pltpu.VMEM((LX, LY), F32),
            pltpu.VMEM((4, LX, LY), F32),
            pltpu.VMEM((DEVICES, WORDS // 2, 128), F32),
            pltpu.VMEM((WORDS * CAP, DEVICES), F32),
            pltpu.VMEM((DEVICES, WORDS // 2, 128), F32),
            pltpu.VMEM((2, 12, GROUP // 2, 128), F32),
            pltpu.VMEM((160, LY), F32),
            pltpu.VMEM((4, 8, 128), F32),
            pltpu.VMEM((4, 8, 128), F32),
            pltpu.SemaphoreType.DMA((6,)),
            pltpu.SemaphoreType.REGULAR((Z,)),
            pltpu.SemaphoreType.DMA,
            pltpu.SemaphoreType.DMA((GROUPS,)),
            pltpu.SemaphoreType.DMA((4,)),
            pltpu.SemaphoreType.DMA((4,)),
        ],
        compiler_params=pltpu.CompilerParams(collective_id=0, has_side_effects=True),
    )(
        parcel_props,
        size_class.reshape(32, 128),
        dest_owner.reshape(32, 128),
        dest_local.reshape(32, 128),
        class_table,
        class_table,
        gas_density,
        gas_rest,
    )
    return pl.pallas_call(
        put_out,
        out_shape=(
            jax.ShapeDtypeStruct((LX, LY), F32),
            jax.ShapeDtypeStruct((4, LX, LY), F32),
        ),
        in_specs=[vmem],
        out_specs=(hbm, hbm),
        scratch_shapes=[pltpu.SemaphoreType.DMA((2,))],
    )(new)


def solution(mesh):
    return jax.shard_map(
        per_device,
        mesh=mesh,
        in_specs=(
            P(None, ("gx", "gy")),
            P(("gx", "gy")),
            P(("gx", "gy"), None),
            P(("gx", "gy")),
            P(),
            P("gx", "gy"),
            P(None, "gx", "gy"),
        ),
        out_specs=(P("gx", "gy"), P(None, "gx", "gy")),
        check_vma=False,
    )
```

```python
import jax
import jax.numpy as jnp
from jax import lax
from jax.experimental import pallas as pl
from jax.experimental.pallas import tpu as pltpu
from jax.sharding import PartitionSpec as P

MESH = pl.DeviceIdType.MESH
F32 = jnp.float32
BF16 = jnp.bfloat16

X, Z, Y, CORES = 4, 8, 4, 2
DEVICES = X * Z * Y * CORES
PARCELS = 4096
CAP = 64
LX, LY = 32, 128
WORDS = 8
STEP = 256
GROUPS = 8
GROUP = DEVICES // GROUPS


PLANES = (0, 1, 7, 2, 6, 3, 5, 4)


def offsets():
    flat = [(dx, dy, dc) for dx in (2, 1, 3, 0) for dy in (2, 1, 3, 0) for dc in range(CORES)]
    return [(dx, dz, dy, dc) for dz in PLANES for dx, dy, dc in flat]


def here():
    gx = lax.axis_index("gx")
    gy = lax.axis_index("gy")
    return gx // Z, gx % Z, gy // CORES, gy % CORES


def peer(at, dx, dz, dy, dc):
    x, z, y, core = at
    return (((x + dx) % X) * Z + (z + dz) % Z, ((y + dy) % Y) * CORES + (core + dc) % CORES)


def signal(sem, to):
    pl.semaphore_signal(sem, inc=1, device_id=to, device_id_type=MESH)


def in_plane(at):
    flat = [(dx, dy, dc) for dx in range(X) for dy in range(Y) for dc in range(CORES)]
    return [peer(at, dx, 0, dy, dc) for dx, dy, dc in flat if dx or dy or dc]


def two_parts(v):
    high = v.astype(BF16).astype(F32)
    return high, v - high


def iota(shape, dim):
    return lax.broadcasted_iota(jnp.int32, shape, dim)


def wide_row(ref, step):
    return jnp.concatenate([ref[2 * step : 2 * step + 1], ref[2 * step + 1 : 2 * step + 2]], axis=1)


def spread(row, height):
    part = jnp.broadcast_to(row, (16, row.shape[1])).astype(BF16)
    return jnp.concatenate([part] * (height // 16), axis=0)


def dot_last(a, b):
    return lax.dot_general(a, b, (((1,), (1,)), ((), ())), preferred_element_type=F32)


def pack(props, classes, owners, locals_, table, blocks, packed, midway):
    across = iota((STEP, STEP), 1)
    down = iota((STEP, STEP), 0)
    earlier = (down < across).astype(F32).astype(BF16)
    ones = jnp.ones((STEP, 128), BF16)
    carry = jnp.zeros((DEVICES, 128), F32)
    columns = jnp.transpose(jnp.concatenate([table[...], jnp.zeros((8, 112), F32)], axis=1))[:16]
    columns = [jnp.broadcast_to(columns[:, k : k + 1], (16, STEP)) for k in range(8)]
    for step in range(PARCELS // STEP):
        if step == 10:
            midway()
        owner = wide_row(owners, step)
        mine = down == owner
        member = jnp.where(mine, 1.0, 0.0).astype(BF16)
        before = jnp.dot(member, earlier, preferred_element_type=F32)
        before = before + jnp.concatenate([carry, carry], axis=1)
        rank = jnp.sum(jnp.where(mine, before, 0.0), axis=0, keepdims=True)
        carry = carry + jnp.dot(member, ones, preferred_element_type=F32)

        q = props[:, step * STEP : (step + 1) * STEP]
        kind = wide_row(classes, step)
        coef = columns[0]
        for k in range(1, 8):
            coef = jnp.where(kind == k, columns[k], coef)
        made = jnp.where(iota((16, STEP), 0) >= 5, coef * q, 0.0)
        energy = q[4:5] + jnp.sum(made, axis=0, keepdims=True)
        local = wide_row(locals_, step).astype(F32)
        words = [q[0:1], q[1:2], q[2:3], q[3:4], q[4:5], energy, kind.astype(F32) + 1.0, local]

        hot = jnp.where(iota((CAP, STEP), 0).astype(F32) == rank, 1.0, 0.0).astype(BF16)
        parts = [two_parts(w) for w in words]
        held = [hot * spread(p[0], CAP) for p in parts] + [hot * spread(p[1], CAP) for p in parts]
        placed = dot_last(jnp.concatenate(held, axis=0), member)
        placed = placed[: WORDS * CAP] + placed[WORDS * CAP :]
        if step:
            packed[...] += placed
        else:
            packed[...] = placed
    for j in range(WORDS // 2):
        blocks[:, j, :] = jnp.transpose(packed[128 * j : 128 * j + 128, :])


def look_up(gas_rows, hi, lo):
    found = [jnp.zeros(hi.shape, F32) for _ in range(5)]
    for h in range(LX):
        at = hi == h
        for k in range(5):
            row = jnp.broadcast_to(gas_rows(k, h), hi.shape)
            found[k] = jnp.where(at, jnp.take_along_axis(row, lo, axis=1, mode="promise_in_bounds"), found[k])
    return found


def sources(words, gas, table):
    q0, q1, q2, q3, q4, energy, kind, _ = words
    coef = []
    for j in range(5):
        c = jnp.full(q0.shape, table[0, j], F32)
        for k in range(1, 8):
            c = jnp.where(kind == k + 1.0, table[k, j], c)
        coef.append(c)
    mass = jnp.where(kind > 0.5, jnp.exp(0.5 * q0), 0.0)
    inverse = 1.0 / gas[0]
    slip = [q - m * inverse for q, m in zip((q1, q2, q3), gas[1:4])]
    warm = q4 - gas[4] * inverse
    rate = coef[0] * (jnp.maximum(warm, 0.0) + jnp.log1p(jnp.exp(-jnp.abs(warm))))
    evapor = mass * (1.0 - jnp.exp(-rate))
    speed = 1.0 + slip[0] * slip[0] + slip[1] * slip[1] + slip[2] * slip[2]
    dragged = mass * (1.0 - jnp.exp(-coef[1] * jnp.sqrt(speed)))
    moment = [evapor * c * q + dragged * w for c, q, w in zip(coef[2:5], (q1, q2, q3), slip)]
    return [evapor, *moment, evapor * energy]


def find_sources(group, recv, gas_rows, table, dense):
    lane = iota((8, 128), 1)
    for half in range(GROUP // 16):
        first = group * GROUP + 16 * half
        words = []
        for j in range(WORDS // 2):
            a = recv[first : first + 8, j, :]
            b = recv[first + 8 : first + 16, j, :]
            words.append(jnp.where(lane < 64, a, pltpu.roll(b, 64, 1)))
            words.append(jnp.where(lane < 64, pltpu.roll(a, 64, 1), b))
        cell = words[7].astype(jnp.int32)
        hi, lo = cell >> 7, cell & 127
        src = sources(words, look_up(gas_rows, hi, lo), table)
        rows = slice(8 * half, 8 * half + 8)
        for k in range(5):
            dense[2 * k, rows], dense[2 * k + 1, rows] = two_parts(src[k])
        dense[10, rows] = hi.astype(F32)
        dense[11, rows] = lo.astype(F32)


def add_sources(group, dense, deposit):
    total = jnp.zeros((320, LY), F32)
    for step in range(GROUP * CAP // STEP):
        at_hi = jnp.where(iota((LX, STEP), 0).astype(F32) == wide_row(dense.at[10], step), 1.0, 0.0).astype(BF16)
        at_lo = jnp.where(iota((LY, STEP), 0).astype(F32) == wide_row(dense.at[11], step), 1.0, 0.0).astype(BF16)
        held = [at_hi * spread(wide_row(dense.at[2 * k + p], step), LX) for p in (0, 1) for k in range(5)]
        total = total + dot_last(jnp.concatenate(held, axis=0), at_lo)
    total = total[:160] + total[160:]
    if group:
        deposit[...] += total
    else:
        deposit[...] = total


def kernel(
    props_h, classes_h, owners_h, locals_h, table, table_s, density_h, rest_h,
    new,
    props, classes, owners, locals_, density, rest, blocks, packed, recv, dense, deposit, edges, halo,
    load_sem, ready, send_sem, recv_sem, edge_sem, halo_sem,
):
    loads = [
        pltpu.make_async_copy(src, dst, load_sem.at[i])
        for i, (src, dst) in enumerate(
            [(owners_h, owners), (props_h, props), (classes_h, classes), (locals_h, locals_), (density_h, density), (rest_h, rest)]
        )
    ]
    for load in loads:
        load.start()
    at = here()
    gx, gy = lax.axis_index("gx"), lax.axis_index("gy")
    barrier = pltpu.get_barrier_semaphore()
    plane = in_plane(at)
    column = [peer(at, 0, dz, 0, 0) for dz in range(1, Z)]
    for to in column + plane:
        signal(barrier, to)

    for load in loads:
        load.wait()

    def midway():
        pl.semaphore_wait(barrier, len(plane) + len(column))
        for dz in range(1, Z):
            signal(ready.at[dz], column[dz - 1])

    pack(props, classes, owners, locals_, table, blocks, packed, midway)

    for slot, off in enumerate(offsets()):
        to = peer(at, *off)
        if slot % GROUP == 0 and off[1]:
            pl.semaphore_wait(ready.at[Z - off[1]], 1)
        if off == (0, 0, 0, 0):
            recv[slot] = blocks[gx * 8 + gy]
        else:
            pltpu.make_async_remote_copy(
                src_ref=blocks.at[to[0] * 8 + to[1]],
                dst_ref=recv.at[slot],
                send_sem=send_sem,
                recv_sem=recv_sem.at[slot // GROUP],
                device_id=to,
                device_id_type=MESH,
            ).start()

    def gas_rows(k, h):
        return density[h : h + 1] if k == 0 else rest[k - 1, h : h + 1]

    def arrived(copies, sem):
        pltpu.make_async_copy(blocks.at[:copies], recv.at[:copies], sem).wait()

    for group in range(GROUPS):
        arrived(GROUP if PLANES[group] else GROUP - 1, recv_sem.at[group])
        if group:
            add_sources(group - 1, dense.at[(group - 1) % 2], deposit)
        find_sources(group, recv, gas_rows, table_s, dense.at[group % 2])
    add_sources(GROUPS - 1, dense.at[(GROUPS - 1) % 2], deposit)
    arrived(DEVICES - 1, send_sem)

    lane = iota((8, 128), 1)
    low_column = jnp.zeros((8, 128), F32)
    high_column = jnp.zeros((8, 128), F32)
    for i in range(20):
        tile = deposit[8 * i : 8 * i + 8]
        low_column = jnp.where(lane == i, pltpu.roll(tile, i, 1) if i else tile, low_column)
        high_column = jnp.where(lane == i, pltpu.roll(tile, i + 1, 1), high_column)
    pad = jnp.zeros((3, 128), F32)
    edges[0] = jnp.concatenate([deposit[32 * k : 32 * k + 1] for k in range(5)] + [pad], axis=0)
    edges[1] = jnp.concatenate([deposit[32 * k + 31 : 32 * k + 32] for k in range(5)] + [pad], axis=0)
    edges[2] = low_column
    edges[3] = high_column
    beside = [
        ((gx + 31) % 32, gy),
        ((gx + 1) % 32, gy),
        (gx, (gy + 7) % 8),
        (gx, (gy + 1) % 8),
    ]
    copies = [
        pltpu.make_async_remote_copy(
            src_ref=edges.at[i],
            dst_ref=halo.at[i],
            send_sem=edge_sem.at[i],
            recv_sem=halo_sem.at[i],
            device_id=to,
            device_id_type=MESH,
        )
        for i, to in enumerate(beside)
    ]
    for copy in copies:
        copy.start()
    for copy in copies:
        copy.wait()

    def kept(value, there):
        return jnp.where(there, value, 0.0)

    above = kept(halo[0], gx < 31)
    below = kept(halo[1], gx > 0)
    right = kept(halo[2], gy < 7)
    left = kept(halo[3], gy > 0)
    for k in range(5):
        field = deposit[32 * k : 32 * k + 32]
        up = jnp.concatenate([field[1:], above[k : k + 1]], axis=0)
        down = jnp.concatenate([below[k : k + 1], field[:-1]], axis=0)
        rights, lefts = [], []
        for i in range(4 * k, 4 * k + 4):
            tile = deposit[8 * i : 8 * i + 8]
            rights.append(jnp.where(lane == 127, pltpu.roll(right, 127 - i, 1), pltpu.roll(tile, 127, 1)))
            lefts.append(jnp.where(lane == 0, pltpu.roll(left, 128 - i, 1) if i else left, pltpu.roll(tile, 1, 1)))
        around = up + down + jnp.concatenate(rights, axis=0) + jnp.concatenate(lefts, axis=0)
        smooth = 0.4 * field + 0.15 * around
        gas = density[...] if k == 0 else rest[k - 1]
        new[k] = gas + smooth


def put_out(new, new_density, new_rest, sem):
    copies = [
        pltpu.make_async_copy(new.at[0], new_density, sem.at[0]),
        pltpu.make_async_copy(new.at[1:], new_rest, sem.at[1]),
    ]
    for copy in copies:
        copy.start()
    for copy in copies:
        copy.wait()


def per_device(parcel_props, size_class, dest_owner, dest_local, class_table, gas_density, gas_rest):
    vmem = pl.BlockSpec(memory_space=pltpu.VMEM)
    hbm = pl.BlockSpec(memory_space=pltpu.HBM)
    smem = pl.BlockSpec(memory_space=pltpu.SMEM)
    new = pl.pallas_call(
        kernel,
        out_shape=jax.ShapeDtypeStruct((5, LX, LY), F32),
        in_specs=[hbm, hbm, hbm, hbm, vmem, smem, hbm, hbm],
        out_specs=vmem,
        scratch_shapes=[
            pltpu.VMEM((16, PARCELS), F32),
            pltpu.VMEM((32, 128), jnp.int32),
            pltpu.VMEM((32, 128), jnp.int32),
            pltpu.VMEM((32, 128), jnp.int32),
            pltpu.VMEM((LX, LY), F32),
            pltpu.VMEM((4, LX, LY), F32),
            pltpu.VMEM((DEVICES, WORDS // 2, 128), F32),
            pltpu.VMEM((WORDS * CAP, DEVICES), F32),
            pltpu.VMEM((DEVICES, WORDS // 2, 128), F32),
            pltpu.VMEM((2, 12, GROUP // 2, 128), F32),
            pltpu.VMEM((160, LY), F32),
            pltpu.VMEM((4, 8, 128), F32),
            pltpu.VMEM((4, 8, 128), F32),
            pltpu.SemaphoreType.DMA((6,)),
            pltpu.SemaphoreType.REGULAR((Z,)),
            pltpu.SemaphoreType.DMA,
            pltpu.SemaphoreType.DMA((GROUPS,)),
            pltpu.SemaphoreType.DMA((4,)),
            pltpu.SemaphoreType.DMA((4,)),
        ],
        compiler_params=pltpu.CompilerParams(collective_id=0, has_side_effects=True),
    )(
        parcel_props,
        size_class.reshape(32, 128),
        dest_owner.reshape(32, 128),
        dest_local.reshape(32, 128),
        class_table,
        class_table,
        gas_density,
        gas_rest,
    )
    return pl.pallas_call(
        put_out,
        out_shape=(
            jax.ShapeDtypeStruct((LX, LY), F32),
            jax.ShapeDtypeStruct((4, LX, LY), F32),
        ),
        in_specs=[vmem],
        out_specs=(hbm, hbm),
        scratch_shapes=[pltpu.SemaphoreType.DMA((2,))],
    )(new)


def solution(mesh):
    return jax.shard_map(
        per_device,
        mesh=mesh,
        in_specs=(
            P(None, ("gx", "gy")),
            P(("gx", "gy")),
            P(("gx", "gy"), None),
            P(("gx", "gy")),
            P(),
            P("gx", "gy"),
            P(None, "gx", "gy"),
        ),
        out_specs=(P("gx", "gy"), P(None, "gx", "gy")),
        check_vma=False,
    )
```
